16 devices in a mesh: dp: 4 (over y, z, core), tp: 4 (over x).
Axes of the slice: x: 4, y: 2, z: 1, core: 2. Of those that a mesh axis runs over, the one named last changes fastest.
The devices are a block of a 4x4x8 slice.
Arguments:
- x: bfloat16 [8192, 6656], P('dp'), parts along dimension 0
- w_gate: bfloat16 [6656, 17920], P(None, 'tp')
- w_up: bfloat16 [6656, 17920], P(None, 'tp')
- w_down: bfloat16 [17920, 6656], P('tp')
Outputs:
- output: bfloat16 [8192, 6656], P('dp'), parts along dimension 0
There are 4 independent parts. The reference program is written for one: setup_inputs(seed, part) draws one part's arguments, and reference() takes and returns one part's arrays. A program takes and returns all parts, laid end to end along the dimension named above; an argument that names none is the same for every part.
All inputs are finite; a program needn't handle non-finite values.
Results may differ from the reference program's by a relative error of at most 0.016.
Values are sent between devices in bfloat16 or wider.
A program may use at most 768 MiB of HBM per device.

```python
import jax
import jax.numpy as jnp

ROWS = 2048
D = 6656
FF = 17920


def setup_inputs(seed: int = 0, part: int = 0) -> dict:
    kx, kg, ku, kd = jax.random.split(jax.random.key(seed), 4)
    drawn = {
        "x": jax.random.normal(jax.random.fold_in(kx, part), (ROWS, D), jnp.float32),
        "w_gate": jax.random.normal(kg, (D, FF), jnp.float32) * D**-0.5,
        "w_up": jax.random.normal(ku, (D, FF), jnp.float32) * D**-0.5,
        "w_down": jax.random.normal(kd, (FF, D), jnp.float32) * FF**-0.5,
    }
    return {k: v.astype(jnp.bfloat16) for k, v in drawn.items()}


def reference(x, w_gate, w_up, w_down):
    gate = jnp.dot(x, w_gate, preferred_element_type=jnp.float32)
    up = jnp.dot(x, w_up, preferred_element_type=jnp.float32)
    hidden = (jax.nn.silu(gate) * up).astype(jnp.bfloat16)
    return jnp.dot(hidden, w_down, preferred_element_type=jnp.float32).astype(jnp.bfloat16)
```

```python
import functools

import jax
import jax.numpy as jnp
from jax import lax
from jax.experimental import pallas as pl
from jax.experimental.pallas import tpu as pltpu
from jax.sharding import PartitionSpec as P

MESH = pl.DeviceIdType.MESH
LANES = 128
PARTS = (5, 6, 7, 8, 6)
SLOTS = 18
WBUF = 3


def kernel(n, sizes, x_ref, wg_ref, wu_ref, wd_ref, y_ref,
           xv, wv, hid, own, s0, s1, fin, rv, xsem, wsem, ssem, rsem, lsem):
    me = lax.axis_index("tp")
    right, left, far = lax.rem(me + 1, n), lax.rem(me + n - 1, n), lax.rem(me + 2, n)
    d, f = wg_ref.shape
    share = d // n
    units = share // LANES
    wide = 2 * LANES
    full, tail = f // wide, f % wide
    tiles = full + (1 if tail else 0)
    steps = tiles + units
    starts = [sum(sizes[:k]) for k in range(len(sizes))]
    last = len(sizes) - 1

    barrier = pltpu.get_barrier_semaphore()
    for nb in (left, right):
        pl.semaphore_signal(barrier, inc=1, device_id={"tp": nb}, device_id_type=MESH)
    pl.semaphore_wait(barrier, 2)

    def wslot(k, q):
        return lax.rem(k * steps + q, WBUF)

    def load_gu(k, i, width):
        b = wslot(k, i)
        c = pl.ds(pl.multiple_of(i * wide, LANES), width)
        return [
            pltpu.make_async_copy(wg_ref.at[:, c], wv.at[b, :, pl.ds(0, width)], wsem.at[b, 0]),
            pltpu.make_async_copy(wu_ref.at[:, c], wv.at[b, :, pl.ds(width, width)], wsem.at[b, 1]),
        ]

    def load_d(k, u):
        b = wslot(k, tiles + u)
        out = []
        for j in range(n):
            owner = lax.rem(me + 1 + j, n)
            c = pl.ds(pl.multiple_of(owner * share + u * LANES, LANES), LANES)
            out.append(pltpu.make_async_copy(
                wd_ref.at[:, c], wv.at[b, pl.ds(0, f), pl.ds(j * LANES, LANES)], wsem.at[b, j]))
        return out

    def start(copies):
        for c in copies:
            c.start()

    def wait(copies):
        for c in copies:
            c.wait()

    def prefetch(k, q):
        if isinstance(q, int):
            if q >= steps:
                if k < last:
                    prefetch(k + 1, q - steps)
            elif q < full:
                start(load_gu(k, q, wide))
            elif q < tiles:
                start(load_gu(k, q, tail))
            else:
                start(load_d(k, q - tiles))
            return

        @pl.when(q < full)
        def _():
            start(load_gu(k, q, wide))

        if tail:
            @pl.when(q == full)
            def _():
                start(load_gu(k, full, tail))

        @pl.when(jnp.logical_and(q >= tiles, q < steps))
        def _():
            start(load_d(k, q - tiles))

        if k < last:
            @pl.when(q >= steps)
            def _():
                start(load_gu(k + 1, q - steps, wide))

    def load_x(k):
        m = sizes[k]
        return pltpu.make_async_copy(x_ref.at[pl.ds(starts[k], m)], xv.at[pl.ds(0, m)], xsem)

    def slot(k, u):
        return lax.rem(k * units + u, SLOTS)

    def cols(owner, u):
        return pl.ds(pl.multiple_of(owner * share + u * LANES, LANES), LANES)

    def remote(src, dst, s, send, recv, to):
        return pltpu.make_async_remote_copy(
            src, dst, ssem.at[send, s], rsem.at[recv, s], device_id={"tp": to}, device_id_type=MESH)

    def first_sends(k, u, js=(0, 1, 2, 3)):
        s, h = slot(k, u), sizes[k] // 2
        r = pl.ds(0, h)
        to = (right, left, left, right)
        return [remote(s0.at[s, j, r], rv.at[j, s, r], s, j, j, to[j]) for j in js]

    def second_sends(k, u):
        s, h = slot(k, u), sizes[k] // 2
        r = pl.ds(0, h)
        return [remote(s1.at[s, j, r], rv.at[4 + j, s, r], s, 4 + j, 4 + j, to)
                for j, to in enumerate((right, left))]

    def rows(k, half=None):
        m = sizes[k]
        if half is None:
            return pl.ds(starts[k], m)
        return pl.ds(starts[k] + half * (m // 2), m // 2)

    def result_sends(k, u, owners):
        s = slot(k, u)
        return [remote(fin.at[s, pl.ds(0, sizes[k])], y_ref.at[rows(k), cols(o, u)], s, 6 + j, 6 + j, to)
                for j, (o, to) in enumerate(zip(owners, (right, left)))]

    def result_local(k, u):
        s = slot(k, u)
        return pltpu.make_async_copy(
            fin.at[s, pl.ds(0, sizes[k])], y_ref.at[rows(k), cols(me, u)], lsem.at[s])

    def relays(k, u, owners):
        s = slot(k, u)
        out = []
        for j, (o, to) in enumerate(zip(owners, (right, left))):
            piece = y_ref.at[rows(k, j), cols(o, u)]
            out.append(remote(piece, piece, s, 8 + j, 8 + j, to))
        return out

    def unit(k, u):
        m = sizes[k]
        h = m // 2
        s = slot(k, u)
        b = wslot(k, tiles + u)
        acc = jnp.dot(hid[pl.ds(0, m)], wv[b, pl.ds(0, f)], preferred_element_type=jnp.float32)
        top, low = acc[:h], acc[h:]

        def part(a, j):
            return a[:, j * LANES:(j + 1) * LANES]

        r = pl.ds(0, h)
        s0[s, 0, r] = part(top, 1).astype(jnp.bfloat16)
        s0[s, 1, r] = part(low, 1).astype(jnp.bfloat16)
        s0[s, 2, r] = part(top, 2).astype(jnp.bfloat16)
        s0[s, 3, r] = part(low, 0).astype(jnp.bfloat16)
        own[s, 0, r] = part(top, 0)
        own[s, 1, r] = part(low, 2)
        own[s, 2, r] = part(top, 3)
        own[s, 3, r] = part(low, 3)
        start(first_sends(k, u))

    def stage1(k, u):
        s, h = slot(k, u), sizes[k] // 2
        r = pl.ds(0, h)
        arrived = first_sends(k, u, (0, 1))
        nxt = second_sends(k, u)
        for j in range(2):
            arrived[j].wait_recv()
            s1[s, j, r] = (rv[j, s, r].astype(jnp.float32) + own[s, j, r]).astype(jnp.bfloat16)
            nxt[j].start()

    def stage2(k, u):
        s, h = slot(k, u), sizes[k] // 2
        r = pl.ds(0, h)
        arrived = first_sends(k, u, (2, 3))
        summed = second_sends(k, u)
        for j in range(2):
            arrived[j].wait_recv()
            summed[j].wait_recv()
            v = rv[4 + j, s, r].astype(jnp.float32) + rv[2 + j, s, r].astype(jnp.float32)
            fin[s, pl.ds(j * h, h)] = (v + own[s, 2 + j, r]).astype(jnp.bfloat16)
        start(result_sends(k, u, (me, me)))
        result_local(k, u).start()
        for c in first_sends(k, u):
            c.wait_send()

    def stage3(k, u):
        arrived = result_sends(k, u, (left, right))
        out = relays(k, u, (left, right))
        for j in range(2):
            arrived[j].wait_recv()
            out[j].start()
        for c in second_sends(k, u):
            c.wait_send()

    def stage4(k, u):
        for c in relays(k, u, (far, far)):
            c.wait_recv()
        for c in result_sends(k, u, (me, me)):
            c.wait_send()
        result_local(k, u).wait()
        for c in relays(k, u, (left, right)):
            c.wait_send()

    def ticks(k, q, plan):
        for stage, (a, span) in zip((stage4, stage3, stage2, stage1), plan[::-1]):
            u = ((q - a) * units) // span if isinstance(q, int) else lax.div(
                jnp.maximum(q - a, 0) * units, span)
            v = ((q + 1 - a) * units) // span if isinstance(q, int) else lax.div(
                jnp.maximum(q + 1 - a, 0) * units, span)
            if isinstance(q, int):
                u, v = max(u, 0), max(v, 0)
                if q >= a and v > u and u < units:
                    stage(k, u)
            else:
                @pl.when(jnp.logical_and(jnp.logical_and(q >= a, v > u), u < units))
                def _():
                    stage(k, u)

    span = max(units, tiles - 3)
    plan = [(0, span), (2, span + 1), (4, span + 2), (6, span + 3)]
    plan_end = [(0, units), (2, units), (4, units), (6, units)]

    load_x(0).start()
    prefetch(0, 0)
    prefetch(0, 1)
    for k, m in enumerate(sizes):
        load_x(k).wait()

        def tile(i, width, k=k, m=m):
            b = wslot(k, i)
            wait(load_gu(k, i, width))
            acc = jnp.dot(xv[pl.ds(0, m)], wv[b, :, pl.ds(0, 2 * width)], preferred_element_type=jnp.float32)
            gate, up = acc[:, :width], acc[:, width:]
            c = pl.ds(pl.multiple_of(i * wide, LANES), width)
            hid[pl.ds(0, m), c] = (jax.nn.silu(gate) * up).astype(jnp.bfloat16)

        @pl.loop(0, full)
        def _(i, k=k):
            prefetch(k, i + 2)
            if k:
                ticks(k - 1, i, plan)
            tile(i, wide)

        if tail:
            prefetch(k, full + 2)
            if k:
                ticks(k - 1, full, plan)
            tile(full, tail)

        if k < last:
            load_x(k + 1).start()

        @pl.loop(0, units)
        def _(u, k=k):
            prefetch(k, tiles + u + 2)
            if k:
                ticks(k - 1, tiles + u, plan)
            wait(load_d(k, u))
            unit(k, u)

    @pl.loop(0, units + 6)
    def _(q):
        ticks(last, q, plan_end)


def solution(mesh):
    n = mesh.shape["tp"]

    def step(x, w_gate, w_up, w_down):
        t, d = x.shape
        f = w_gate.shape[1]
        sizes = [t * p // sum(PARTS) for p in PARTS]
        top = max(sizes)
        half = top // 2
        hbm = [pltpu.with_memory_space_constraint(a, pltpu.HBM) for a in (x, w_gate, w_up, w_down)]
        bf = jnp.bfloat16
        return pl.pallas_call(
            functools.partial(kernel, n, sizes),
            out_shape=jax.ShapeDtypeStruct((t, d), bf),
            in_specs=[pl.BlockSpec(memory_space=pltpu.HBM)] * 4,
            out_specs=pl.BlockSpec(memory_space=pltpu.HBM),
            scratch_shapes=[
                pltpu.VMEM((top, d), bf),
                pltpu.VMEM((WBUF, max(d, f), 4 * LANES), bf),
                pltpu.VMEM((top, f), bf),
                pltpu.VMEM((SLOTS, 4, half, LANES), jnp.float32),
                pltpu.VMEM((SLOTS, 4, half, LANES), bf),
                pltpu.VMEM((SLOTS, 2, half, LANES), bf),
                pltpu.VMEM((SLOTS, top, LANES), bf),
                pltpu.VMEM((6, SLOTS, half, LANES), bf),
                pltpu.SemaphoreType.DMA,
                pltpu.SemaphoreType.DMA((WBUF, 4)),
                pltpu.SemaphoreType.DMA((10, SLOTS)),
                pltpu.SemaphoreType.DMA((10, SLOTS)),
                pltpu.SemaphoreType.DMA((SLOTS,)),
            ],
            name="mlp",
            compiler_params=pltpu.CompilerParams(
                collective_id=0, has_side_effects=True, vmem_limit_bytes=67043328),
            cost_estimate=pl.CostEstimate(flops=6 * t * d * f, bytes_accessed=6 * d * f, transcendentals=t * f),
        )(*hbm)

    return jax.shard_map(
        step,
        mesh=mesh,
        in_specs=(P("dp", None), P(None, "tp"), P(None, "tp"), P("tp", None)),
        out_specs=P("dp", None),
        check_vma=False,
    )
```

```python
import functools

import jax
import jax.numpy as jnp
from jax import lax
from jax.experimental import pallas as pl
from jax.experimental.pallas import tpu as pltpu
from jax.sharding import PartitionSpec as P

MESH = pl.DeviceIdType.MESH
LANES = 128
PARTS = (11, 11, 11, 11, 11, 9)
HELD = 4
PLAN = ((0, 13), (3, 14), (6, 18), (11, 19))
LAST = ((4, 13), (8, 13), (15, 13), (19, 20))
SLOTS = 16
WBUF = 3
VMEM = 66 * 10**6


def kernel(n, sizes, x_ref, wg_ref, wu_ref, wd_ref, y_ref, yv_ref,
           xv, wv, hid, own, s0, s1, fin, rv, xsem, wsem, ssem, rsem, lsem):
    me = lax.axis_index("tp")
    right, left, far = lax.rem(me + 1, n), lax.rem(me + n - 1, n), lax.rem(me + 2, n)
    d, f = wg_ref.shape
    share = d // n
    units = share // LANES
    wide = 2 * LANES
    full, tail = f // wide, f % wide
    tiles = full + (1 if tail else 0)
    steps = tiles + units
    starts = [sum(sizes[:k]) for k in range(len(sizes))]
    last = len(sizes) - 1
    held = len(sizes) - HELD

    plan = [(a, b * units // 13) for a, b in PLAN]
    end = [(a, b * units // 13) for a, b in LAST]

    def wslot(k, q):
        return lax.rem(k * steps + q, WBUF)

    def load_gu(k, i, width):
        b = wslot(k, i)
        c = pl.ds(pl.multiple_of(i * wide, LANES), width)
        return [
            pltpu.make_async_copy(wg_ref.at[:, c], wv.at[b, :, pl.ds(0, width)], wsem.at[b, 0]),
            pltpu.make_async_copy(wu_ref.at[:, c], wv.at[b, :, pl.ds(width, width)], wsem.at[b, 1]),
        ]

    def load_d(k, u):
        b = wslot(k, tiles + u)
        out = []
        for j in range(n):
            owner = lax.rem(me + 1 + j, n)
            c = pl.ds(pl.multiple_of(owner * share + u * LANES, LANES), LANES)
            out.append(pltpu.make_async_copy(
                wd_ref.at[:, c], wv.at[b, pl.ds(0, f), pl.ds(j * LANES, LANES)], wsem.at[b, j]))
        return out

    def start(copies):
        for c in copies:
            c.start()

    def wait(copies):
        for c in copies:
            c.wait()

    def prefetch(k, q, first=0):
        if isinstance(q, int):
            if q >= steps:
                if k < last:
                    prefetch(k + 1, q - steps)
            elif q < full:
                start(load_gu(k, q, wide))
            elif q < tiles:
                start(load_gu(k, q, tail))
            else:
                start(load_d(k, q - tiles))
            return

        if not first:
            @pl.when(q < full)
            def _():
                start(load_gu(k, q, wide))

        if tail and not first:
            @pl.when(q == full)
            def _():
                start(load_gu(k, full, tail))

        @pl.when(jnp.logical_and(q >= tiles, q < steps))
        def _():
            start(load_d(k, q - tiles))

        if first and k < last:
            @pl.when(q >= steps)
            def _():
                start(load_gu(k + 1, q - steps, wide))

    def load_x(k):
        m = sizes[k]
        return pltpu.make_async_copy(x_ref.at[pl.ds(starts[k], m)], xv.at[pl.ds(0, m)], xsem)

    def slot(k, u):
        return lax.rem(k * units + u, SLOTS)

    def cols(owner, u):
        return pl.ds(pl.multiple_of(owner * share + u * LANES, LANES), LANES)

    def remote(src, dst, s, send, recv, to):
        return pltpu.make_async_remote_copy(
            src, dst, ssem.at[send, s], rsem.at[recv, s], device_id={"tp": to}, device_id_type=MESH)

    def first_sends(k, u, js=(0, 1, 2, 3)):
        s, h = slot(k, u), sizes[k] // 2
        r = pl.ds(0, h)
        to = (right, left, left, right)
        return [remote(s0.at[s, j, r], rv.at[j, s, r], s, j, j, to[j]) for j in js]

    def second_sends(k, u):
        s, h = slot(k, u), sizes[k] // 2
        r = pl.ds(0, h)
        return [remote(s1.at[s, j, r], rv.at[4 + j, s, r], s, 4 + j, 4 + j, to)
                for j, to in enumerate((right, left))]

    def piece(k, owner, u, half=None):
        m = sizes[k]
        ref, at = (y_ref, starts[k]) if k < held else (yv_ref, starts[k] - starts[held])
        r = pl.ds(at, m) if half is None else pl.ds(at + half * (m // 2), m // 2)
        return ref.at[r, cols(owner, u)]

    def result_sends(k, u, owners):
        s = slot(k, u)
        out = []
        for j, (o, to) in enumerate(zip(owners, (right, left))):
            dst = piece(k, o, u)
            src = fin.at[s, pl.ds(0, sizes[k])] if k < held else dst
            out.append(remote(src, dst, s, 6 + j, 6 + j, to))
        return out

    def result_local(k, u):
        s = slot(k, u)
        return pltpu.make_async_copy(fin.at[s, pl.ds(0, sizes[k])], piece(k, me, u), lsem.at[s])

    def relays(k, u, owners):
        s = slot(k, u)
        out = []
        for j, (o, to) in enumerate(zip(owners, (right, left))):
            p = piece(k, o, u, j)
            out.append(remote(p, p, s, 8 + j, 8 + j, to))
        return out

    def unit(k, u):
        m = sizes[k]
        h = m // 2
        s = slot(k, u)
        b = wslot(k, tiles + u)
        acc = jnp.dot(hid[pl.ds(0, m)], wv[b, pl.ds(0, f)], preferred_element_type=jnp.float32)
        top, low = acc[:h], acc[h:]

        def part(a, j):
            return a[:, j * LANES:(j + 1) * LANES]

        r = pl.ds(0, h)
        s0[s, 0, r] = part(top, 1).astype(jnp.bfloat16)
        s0[s, 1, r] = part(low, 1).astype(jnp.bfloat16)
        s0[s, 2, r] = part(top, 2).astype(jnp.bfloat16)
        s0[s, 3, r] = part(low, 0).astype(jnp.bfloat16)
        own[s, 0, r] = part(top, 0)
        own[s, 1, r] = part(low, 2)
        own[s, 2, r] = part(top, 3)
        own[s, 3, r] = part(low, 3)
        start(first_sends(k, u))

    def stage1(k, u):
        s, h = slot(k, u), sizes[k] // 2
        r = pl.ds(0, h)
        arrived = first_sends(k, u, (0, 1))
        nxt = second_sends(k, u)
        for j in range(2):
            arrived[j].wait_recv()
            s1[s, j, r] = (rv[j, s, r].astype(jnp.float32) + own[s, j, r]).astype(jnp.bfloat16)
            nxt[j].start()

    def stage2(k, u):
        s, h = slot(k, u), sizes[k] // 2
        r = pl.ds(0, h)
        arrived = first_sends(k, u, (2, 3))
        summed = second_sends(k, u)
        for j in range(2):
            arrived[j].wait_recv()
            summed[j].wait_recv()
            v = rv[4 + j, s, r].astype(jnp.float32) + rv[2 + j, s, r].astype(jnp.float32)
            v = (v + own[s, 2 + j, r]).astype(jnp.bfloat16)
            if k < held:
                fin[s, pl.ds(j * h, h)] = v
            else:
                yv_ref[pl.ds(starts[k] - starts[held] + j * h, h), cols(me, u)] = v
        start(result_sends(k, u, (me, me)))
        if k < held:
            result_local(k, u).start()
        for c in first_sends(k, u):
            c.wait_send()

    def stage3(k, u):
        arrived = result_sends(k, u, (left, right))
        out = relays(k, u, (left, right))
        for j in range(2):
            arrived[j].wait_recv()
            out[j].start()
        for c in second_sends(k, u):
            c.wait_send()

    def stage4(k, u):
        for c in relays(k, u, (far, far)):
            c.wait_recv()
        for c in result_sends(k, u, (me, me)):
            c.wait_send()
        if k < held:
            result_local(k, u).wait()
        for c in relays(k, u, (left, right)):
            c.wait_send()

    def ticks(k, q, plan):
        for stage, (a, span) in zip((stage4, stage3, stage2, stage1), plan[::-1]):
            u = ((q - a) * units) // span if isinstance(q, int) else lax.div(
                jnp.maximum(q - a, 0) * units, span)
            v = ((q + 1 - a) * units) // span if isinstance(q, int) else lax.div(
                jnp.maximum(q + 1 - a, 0) * units, span)
            if isinstance(q, int):
                u, v = max(u, 0), max(v, 0)
                if q >= a and v > u and u < units:
                    stage(k, u)
            else:
                @pl.when(jnp.logical_and(jnp.logical_and(q >= a, v > u), u < units))
                def _():
                    stage(k, u)

    load_x(0).start()
    prefetch(0, 0)
    prefetch(0, 1)
    barrier = pltpu.get_barrier_semaphore()
    for nb in (left, right):
        pl.semaphore_signal(barrier, inc=1, device_id={"tp": nb}, device_id_type=MESH)
    pl.semaphore_wait(barrier, 2)

    for k, m in enumerate(sizes):
        load_x(k).wait()

        def tile(i, width, k=k, m=m):
            b = wslot(k, i)
            wait(load_gu(k, i, width))
            acc = jnp.dot(xv[pl.ds(0, m)], wv[b, :, pl.ds(0, 2 * width)], preferred_element_type=jnp.float32)
            gate, up = acc[:, :width], acc[:, width:]
            c = pl.ds(pl.multiple_of(i * wide, LANES), width)
            hid[pl.ds(0, m), c] = (jax.nn.silu(gate) * up).astype(jnp.bfloat16)

        @pl.loop(0, full)
        def _(i, k=k):
            prefetch(k, i + 2)
            if k:
                ticks(k - 1, i, plan)
            tile(i, wide)

        if tail:
            prefetch(k, full + 2)
            if k:
                ticks(k - 1, full, plan)
            tile(full, tail)

        if k < last:
            load_x(k + 1).start()

        @pl.loop(0, units)
        def _(u, k=k):
            prefetch(k, tiles + u + 2, tiles)
            if k:
                ticks(k - 1, tiles + u, plan)
            if k == last:
                ticks(k, u, end)
            wait(load_d(k, u))
            unit(k, u)

    @pl.loop(units, max(a + b for a, b in end))
    def _(q):
        ticks(last, q, end)


def join(cuts, a_ref, b_ref, y_ref, buf, isem, osem, bsem):
    n, m = a_ref.shape[0], b_ref.shape[0]
    loads, stores, rest = [], [], []
    for i in range(cuts):
        r = pl.ds(i * (n // cuts), n // cuts)
        loads.append(pltpu.make_async_copy(a_ref.at[r], buf.at[r], isem.at[i]))
        stores.append(pltpu.make_async_copy(buf.at[r], y_ref.at[r], osem.at[i]))
        p = m // cuts
        rest.append(pltpu.make_async_copy(
            b_ref.at[pl.ds(i * p, p)], y_ref.at[pl.ds(n + i * p, p)], bsem.at[i]))
    for c in loads:
        c.start()
    for c in rest:
        c.start()
    for c, o in zip(loads, stores):
        c.wait()
        o.start()
    for c in stores + rest:
        c.wait()


def solution(mesh):
    n = mesh.shape["tp"]

    def step(x, w_gate, w_up, w_down):
        t, d = x.shape
        f = w_gate.shape[1]
        sizes = [t * p // sum(PARTS) for p in PARTS]
        top = max(sizes)
        half = top // 2
        hbm = [pltpu.with_memory_space_constraint(a, pltpu.HBM) for a in (x, w_gate, w_up, w_down)]
        bf = jnp.bfloat16
        split = sum(sizes[:-HELD])
        part, kept = pl.pallas_call(
            functools.partial(kernel, n, sizes),
            out_shape=(jax.ShapeDtypeStruct((split, d), bf), pltpu.VMEM((t - split, d), bf)),
            in_specs=[pl.BlockSpec(memory_space=pltpu.HBM)] * 4,
            out_specs=(pl.BlockSpec(memory_space=pltpu.HBM), pl.BlockSpec(memory_space=pltpu.VMEM)),
            scratch_shapes=[
                pltpu.VMEM((top, d), bf),
                pltpu.VMEM((WBUF, max(d, f), 4 * LANES), bf),
                pltpu.VMEM((top, f), bf),
                pltpu.VMEM((SLOTS, 4, half, LANES), jnp.float32),
                pltpu.VMEM((SLOTS, 4, half, LANES), bf),
                pltpu.VMEM((SLOTS, 2, half, LANES), bf),
                pltpu.VMEM((SLOTS, top, LANES), bf),
                pltpu.VMEM((6, SLOTS, half, LANES), bf),
                pltpu.SemaphoreType.DMA,
                pltpu.SemaphoreType.DMA((WBUF, 4)),
                pltpu.SemaphoreType.DMA((10, SLOTS)),
                pltpu.SemaphoreType.DMA((10, SLOTS)),
                pltpu.SemaphoreType.DMA((SLOTS,)),
            ],
            name="mlp",
            compiler_params=pltpu.CompilerParams(
                collective_id=0, has_side_effects=True, vmem_limit_bytes=VMEM - (t - split) * d * 2),
            cost_estimate=pl.CostEstimate(flops=6 * t * d * f, bytes_accessed=6 * d * f, transcendentals=t * f),
        )(*hbm)
        cuts = 4
        part = pltpu.with_memory_space_constraint(part, pltpu.HBM)
        kept = pltpu.with_memory_space_constraint(kept, pltpu.VMEM)
        return pl.pallas_call(
            functools.partial(join, cuts),
            out_shape=jax.ShapeDtypeStruct((t, d), bf),
            in_specs=[pl.BlockSpec(memory_space=pltpu.HBM), pl.BlockSpec(memory_space=pltpu.VMEM)],
            out_specs=pl.BlockSpec(memory_space=pltpu.HBM),
            scratch_shapes=[pltpu.VMEM((split, d), bf)] + [pltpu.SemaphoreType.DMA((cuts,))] * 3,
            name="join",
            compiler_params=pltpu.CompilerParams(vmem_limit_bytes=split * d * 2 + (4 << 20)),
        )(part, kept)

    return jax.shard_map(
        step,
        mesh=mesh,
        in_specs=(P("dp", None), P(None, "tp"), P(None, "tp"), P("tp", None)),
        out_specs=P("dp", None),
        check_vma=False,
    )
```
